32 devices in a mesh: dp: 4 (over y, x), ctx: 8 (over z, core).
Axes of the slice: x: 2, y: 2, z: 4, core: 2. Of those that a mesh axis runs over, the one named last changes fastest.
Arguments:
- tokens: bfloat16 [4, 3072, 1024], P('dp', 'ctx'), may hold values from -6 to 6
- modality: int32 [4, 3072], P('dp', 'ctx'), may hold values 0 or 1
- type_embed: bfloat16 [2, 1024], replicated, may hold values from -6 to 6
- dest_shard: int32 [4, 3072], P('dp'), may hold values from 0 to 7, as said below
- dest_row: int32 [4, 3072], P('dp'), may hold values from 0 to 383, as said below
- segments: int32 [4, 3072], P('dp'), may hold values from 0 to 15, never falling along the last dimension, each value on 1 to 384 neighbouring positions
- w_qkv: bfloat16 [1024, 3072], P('ctx', 'dp')
- w_out: bfloat16 [1024, 1024], P('ctx', 'dp'), may hold values from -0.1875 to 0.1875
- w_up: bfloat16 [1024, 2048], P('ctx', 'dp'), may hold values from -0.1875 to 0.1875
- w_down: bfloat16 [2048, 1024], P('ctx', 'dp'), may hold values from -0.125 to 0.125
Outputs:
- encoded: bfloat16 [4, 3072, 1024], P('dp', 'ctx')
The draws below stay inside these ranges and needn't reach their ends.
Inputs may be any that keep to these rules, and one draw needn't show every extreme that they name: For each sequence, dest_shard and dest_row together map its 3072 tokens one to one onto the 3072 packed positions. Among the tokens of one device (aligned blocks of 384), at most 96 have the same dest_shard, and in every draw some block has exactly 96 for some shard. `dest_row`: see dest_shard. `segments`: segment numbers never fall along a sequence; each segment holds 1 to 384 positions.
All inputs are finite; a program needn't handle non-finite values. No bound on the sum of `modality` on one device may be relied on, other than what follows from the above.
Results may differ from the reference program's by a relative error of at most 0.006.
Values may be sent and summed in bfloat16 or wider, within the bound.
No kernel may reach another device: no remote copies, remote signals or barrier semaphores. Data moves between devices by JAX's collectives and lax.ppermute only.
A program may use at most 128 MiB of HBM per device.

```python
import math
import jax
import jax.numpy as jnp
import numpy as np
from jax import lax

D = 1024
HEADS = 16
FF = 2048
SEQ_DEV = 384
SEQ = 3072
BATCH = 4
CAP = 96
N_CTX = 8


def one_plan(seed_key):
    shards = SEQ // SEQ_DEV
    half_cap = CAP // 2
    key_a, key_b, key_c, key_d, key_e = jax.random.split(seed_key, 5)
    pairing = jax.random.permutation(key_a, shards)
    moved = jax.random.randint(key_b, (shards // 2,), 0, half_cap + 1).at[0].set(half_cap)
    loads = jnp.full((shards,), half_cap, jnp.int32).at[pairing[0::2]].add(moved).at[pairing[1::2]].add(-moved)
    offsets = jax.random.permutation(key_c, shards)
    sources = jnp.arange(shards, dtype=jnp.int32)
    targets = (sources[:, None] + offsets[None, :]) % shards
    source_grid = jnp.broadcast_to(sources[:, None], (shards, shards))
    counts = jnp.zeros((shards, shards), jnp.int32).at[source_grid, targets].add(jnp.broadcast_to(loads[None, :], (shards, shards)))
    bounds = jnp.cumsum(counts, axis=1)
    ranks = jnp.arange(SEQ_DEV, dtype=jnp.int32)
    sorted_dest = jnp.sum((bounds[:, None, :] <= ranks[None, :, None]).astype(jnp.int32), axis=2)
    shuffles = jax.vmap(lambda sub_key: jax.random.permutation(sub_key, SEQ_DEV))(jax.random.split(key_d, shards))
    plan_shard = jnp.take_along_axis(sorted_dest, shuffles, axis=1).reshape(-1)
    chosen = (plan_shard[:, None] == sources[None, :]).astype(jnp.int32)
    arrival = jnp.sum((jnp.cumsum(chosen, axis=0) - chosen) * chosen, axis=1)
    placements = jax.vmap(lambda sub_key: jax.random.permutation(sub_key, SEQ_DEV))(jax.random.split(key_e, shards))
    plan_row = placements[plan_shard, arrival]
    return (plan_shard.astype(jnp.int32), plan_row.astype(jnp.int32))


def packing_plan(key):
    plan_key = jax.random.fold_in(key, 17)
    return jax.vmap(one_plan)(jax.random.split(plan_key, BATCH))


def draw_dest_shard(key, part):
    return packing_plan(key)[0]


def draw_dest_row(key, part):
    return packing_plan(key)[1]


def draw_w_qkv(key, part):
    key_a = jax.random.fold_in(jax.random.fold_in(key, 29), 0)
    base = jax.random.normal(key_a, (D, 3 * D), jnp.float32) / jnp.sqrt(jnp.float32(D))
    return base.astype(jnp.bfloat16)


def plant(values, key, least, top_value):
    longest = values.shape.index(max(values.shape))
    spots = []
    for shift in (0, 1):
        where = [jax.random.randint(jax.random.fold_in(key, axis), (), 0, length) for axis, length in enumerate(values.shape)]
        where[longest] = (where[longest] + shift) % values.shape[longest]
        spots.append(tuple(where))
    return values.at[spots[0]].set(least).at[spots[1]].set(top_value)


def block_levels(key, extent, pieces, low, top_value):
    def one(dim, shards_of):
        draws = jax.random.uniform(jax.random.fold_in(jax.random.fold_in(key, 6), dim), (shards_of,), jnp.float32, low / len(pieces), top_value / len(pieces))
        return jnp.repeat(jnp.exp(draws), extent[dim] // shards_of).reshape((-1,) + (1,) * (len(extent) - dim - 1))

    loudness = one(*pieces[0])
    for cut in pieces[1:]:
        loudness = loudness * one(*cut)
    return loudness


def split_up(number_of, total, bound, skew):
    weights = [(1 << 20) // math.isqrt(rank ** skew) + 1 for rank in range(2, number_of + 1)]
    surplus, given = total - bound - (number_of - 1), [1] * (number_of - 1)
    while surplus > 0:
        free = [i for i in range(number_of - 1) if given[i] < bound]
        whole, remaining = sum([weights[i] for i in free]), surplus
        for i in free:
            more = min(bound - given[i], max(1, remaining * weights[i] // whole), surplus)
            given[i] = given[i] + more
            surplus = surplus - more
    return np.array([bound] + given)


def uneven_parts(own_key, number_of, total, reach, lean):
    if number_of == 2:
        one = jax.random.randint(own_key, (), max(1, total - reach), min(reach, total - 1) + 1)
        return jnp.stack([one, total - one])
    sizes = jnp.asarray(split_up(number_of, total, reach, lean), jnp.int32)
    couples = (number_of - 1) // 2
    donor, sink = sizes[1:1 + 2 * couples:2], sizes[2:2 + 2 * couples:2]
    slack = jnp.minimum(donor - 1, reach - sink)
    moved = jax.random.randint(jax.random.fold_in(own_key, 1), (couples,), 0, 1 << 20) % (slack + 1)
    sizes = sizes.at[1:1 + 2 * couples:2].set(donor - moved).at[2:2 + 2 * couples:2].set(sink + moved)
    return sizes[jax.random.permutation(jax.random.fold_in(own_key, 2), number_of)]


def centred(stream_key, extent, scale, bound, cuts=(), held_as=jnp.bfloat16):
    values = scale * jax.random.normal(stream_key, extent, jnp.float32)
    if cuts:
        values = values * block_levels(stream_key, extent, cuts, -0.22, 0.18)
    return jnp.clip(values, -bound, bound).astype(held_as)


def setup_inputs(seed: int = 0) -> dict:
    key_of = jax.random.split(jax.random.key(seed), 11)
    return {
        "tokens": centred(key_of[0], (BATCH, SEQ, D), 1.0, 6.0, ((0, 4), (1, 8))),
        "modality": plant((jax.random.randint(key_of[1], (BATCH, SEQ), 0, 3) < 1).astype(jnp.int32), jax.random.fold_in(key_of[1], 1), 0, 1),
        "type_embed": centred(key_of[2], (2, D), 1.0, 6.0),
        "dest_shard": draw_dest_shard(jax.random.fold_in(key_of[10], 71), 0),
        "dest_row": draw_dest_row(jax.random.fold_in(key_of[10], 71), 0),
        "segments": jax.vmap(lambda own: jnp.searchsorted(jnp.cumsum(uneven_parts(own, 2 * SEQ // SEQ_DEV, SEQ, SEQ_DEV, 0)), jnp.arange(SEQ), side="right"))(jax.random.split(key_of[5], BATCH)).reshape((BATCH, SEQ)).astype(jnp.int32),
        "w_qkv": draw_w_qkv(jax.random.fold_in(key_of[10], 71), 0),
        "w_out": centred(key_of[7], (D, D), D ** -0.5, 0.1875, ((0, 8), (1, 4))),
        "w_up": centred(key_of[8], (D, FF), D ** -0.5, 0.1875, ((0, 8), (1, 4))),
        "w_down": centred(key_of[9], (FF, D), FF ** -0.5, 0.125, ((0, 8), (1, 4))),
    }


norm_eps = 1e-06

def layer_norm(values):
    row_mean = lax.optimization_barrier(jnp.mean(values, axis=-1, keepdims=True))
    centered = values - row_mean
    spread = lax.optimization_barrier(jnp.mean(centered * centered, axis=-1, keepdims=True))
    return centered * lax.rsqrt(spread + norm_eps)

def attend(queries, key_pairs, query_seg, key_seg):
    seq_rows = queries.shape[0]
    key_span = key_pairs.shape[0]
    head_dim = D // HEADS
    query_heads = queries.reshape(seq_rows, HEADS, head_dim).astype(jnp.float32)
    key_heads = key_pairs[:, :D].reshape(key_span, HEADS, head_dim).astype(jnp.float32)
    value_heads = key_pairs[:, D:].reshape(key_span, HEADS, head_dim).astype(jnp.float32)
    allowed = query_seg[:, None] == key_seg[None, :]
    scores = jnp.einsum('qhd,khd->hqk', query_heads, key_heads) * head_dim ** (-0.5)
    scores = jnp.where(allowed[None], scores, -1e+30)
    row_max = lax.optimization_barrier(jnp.max(scores, axis=-1, keepdims=True))
    expd = jnp.exp(scores - row_max)
    attn_probs = (expd / lax.optimization_barrier(jnp.sum(expd, axis=-1, keepdims=True))).astype(jnp.bfloat16)
    head_mix = jnp.einsum('hqk,khd->qhd', attn_probs.astype(jnp.float32), value_heads)
    return head_mix.reshape(seq_rows, D).astype(jnp.bfloat16)

def encode(embedded, plan_shard, plan_row, seq_seg, w_qkv, w_out, w_up, w_down):
    place = plan_shard * SEQ_DEV + plan_row
    packed = jnp.zeros((SEQ, D), jnp.bfloat16).at[place].set(embedded)
    normed = layer_norm(packed.astype(jnp.float32)).astype(jnp.bfloat16)
    qkv_all = jnp.dot(normed, w_qkv, preferred_element_type=jnp.float32).astype(jnp.bfloat16)
    queries = qkv_all[:, :D]
    empty_rim = jnp.zeros((SEQ_DEV, 2 * D), jnp.bfloat16)
    key_pairs = jnp.concatenate([empty_rim, qkv_all[:, D:], empty_rim], axis=0)
    filler = jnp.full((SEQ_DEV,), -1, jnp.int32)
    padded_seg = jnp.concatenate([filler, seq_seg, filler])

    def one_block(block_index):
        offset = (block_index * SEQ_DEV).astype(jnp.int32)
        q_block = lax.dynamic_slice_in_dim(queries, offset, SEQ_DEV, 0)
        kv_block = lax.dynamic_slice_in_dim(key_pairs, offset, 3 * SEQ_DEV, 0)
        query_seg = lax.dynamic_slice_in_dim(seq_seg, offset, SEQ_DEV, 0)
        key_seg = lax.dynamic_slice_in_dim(padded_seg, offset, 3 * SEQ_DEV, 0)
        return attend(q_block, kv_block, query_seg, key_seg)
    attended = lax.map(one_block, jnp.arange(N_CTX, dtype=jnp.int32)).reshape(SEQ, D)
    middle = packed.astype(jnp.float32) + jnp.dot(attended, w_out, preferred_element_type=jnp.float32)
    normed_mid = layer_norm(middle).astype(jnp.bfloat16)
    hidden = jax.nn.gelu(jnp.dot(normed_mid, w_up, preferred_element_type=jnp.float32), approximate=True).astype(jnp.bfloat16)
    result = (middle + jnp.dot(hidden, w_down, preferred_element_type=jnp.float32)).astype(jnp.bfloat16)
    return result[place]

def reference(tokens, modality, type_embed, dest_shard, dest_row, segments, w_qkv, w_out, w_up, w_down):
    extra = jnp.where(modality[:, :, None] == 1, type_embed[1], type_embed[0]).astype(jnp.float32)
    embedded = (tokens.astype(jnp.float32) + extra).astype(jnp.bfloat16)
    outputs = []
    for seq_index in range(BATCH):
        outputs.append(encode(embedded[seq_index], dest_shard[seq_index], dest_row[seq_index], segments[seq_index], w_qkv, w_out, w_up, w_down))
    return jnp.stack(outputs)
```

```python
import functools

import jax
import jax.numpy as jnp
from jax import lax
from jax.experimental import pallas as pl
from jax.experimental.pallas import tpu as pltpu
from jax.sharding import PartitionSpec as P


HEADS = 16


norm_eps = 1e-06


def extended(value, sides, width):
    for axis, dim in sides:
        devices, length = (lax.axis_size(axis), value.shape[dim])
        up = [(i, (i + 1) % devices) for i in range(devices - 1)]
        down = [(j, i) for i, j in up]
        last = lax.slice_in_dim(value, length - width, length, axis=dim)
        initial = lax.slice_in_dim(value, 0, width, axis=dim)
        before = lax.ppermute(last, axis, up)
        after = lax.ppermute(initial, axis, down)
        value = jnp.concatenate([before, value, after], axis=dim)
    return value


def layer_norm(values):
    row_mean = jnp.mean(values, axis=-1, keepdims=True)
    centered = values - row_mean
    spread = jnp.mean(centered * centered, axis=-1, keepdims=True)
    return centered * lax.rsqrt(spread + norm_eps)


def attend(queries, key_pairs, query_seg, key_seg, head_count):
    seq_rows, model_width = queries.shape
    key_span = key_pairs.shape[0]
    groups = head_count // 4
    head_dim = model_width // head_count
    query_groups = queries.reshape(seq_rows, groups, 4, head_dim).transpose(1, 0, 2, 3)
    key_groups = (
        key_pairs[:, :model_width].reshape(key_span, groups, 4, head_dim).transpose(1, 0, 2, 3)
    )
    value_groups = (
        key_pairs[:, model_width:].reshape(key_span, groups, 4, head_dim).transpose(1, 0, 2, 3)
    )
    allowed = query_seg[:, None] == key_seg[None, :]
    score_scale = head_dim ** (-0.5)

    def one_group(operands):
        query_part, key_part, value_part = operands
        scores = (
            jnp.einsum("qhd,khd->hqk", query_part, key_part, preferred_element_type=jnp.float32)
            * score_scale
        )
        scores = jnp.where(allowed[None], scores, -1e30)
        row_max = jnp.max(scores, axis=-1, keepdims=True)
        expd = jnp.exp(scores - row_max)
        attn_probs = (expd / jnp.sum(expd, axis=-1, keepdims=True)).astype(jnp.bfloat16)
        return jnp.einsum(
            "hqk,khd->qhd", attn_probs, value_part, preferred_element_type=jnp.float32
        )

    head_mix = lax.map(one_group, (query_groups, key_groups, value_groups))
    return head_mix.transpose(1, 0, 2, 3).reshape(seq_rows, model_width).astype(jnp.bfloat16)


def packed_layer(tokens, modality, type_embed, dest_shard, dest_row, segments, w_qkv, w_out, w_up, w_down):
    shards = lax.axis_size("ctx")
    own_index = lax.axis_index("ctx")
    seq_rows = tokens.shape[1]
    model_width = tokens.shape[2]
    capacity = 2 * seq_rows // shards
    slot_total = shards * capacity
    extra = jnp.where(modality[0][:, None] == 1, type_embed[1], type_embed[0]).astype(jnp.float32)
    embedded = (tokens[0].astype(jnp.float32) + extra).astype(jnp.bfloat16)
    plan_shard = dest_shard[0].reshape(shards, seq_rows)
    plan_row = dest_row[0].reshape(shards, seq_rows)
    owners = jnp.arange(shards, dtype=jnp.int32)
    row_ids = jnp.arange(seq_rows, dtype=jnp.int32)
    slot_ids = jnp.arange(slot_total, dtype=jnp.int32)
    before = (row_ids[:, None] > row_ids[None, :]).astype(jnp.bfloat16)
    own_plan = lax.dynamic_index_in_dim(plan_shard, own_index, 0, keepdims=False)
    chosen = own_plan[:, None] == owners[None, :]
    earlier_all = jnp.dot(before, chosen.astype(jnp.bfloat16), preferred_element_type=jnp.float32)
    earlier = jnp.sum(jnp.where(chosen, earlier_all, 0.0), axis=1).astype(jnp.int32)
    outgoing_slot = own_plan * capacity + earlier
    slot_hit = outgoing_slot[None, :] == slot_ids[:, None]
    slot_token = jnp.sum(jnp.where(slot_hit, row_ids[None, :], 0), axis=1)
    slot_full = jnp.any(slot_hit, axis=1)
    outbox_rows = jnp.where(slot_full[:, None], embedded[slot_token], jnp.zeros((), jnp.bfloat16))
    inbox_rows = lax.all_to_all(
        outbox_rows.reshape(shards, capacity, model_width),
        "ctx",
        split_axis=0,
        concat_axis=0,
        tiled=True,
    )
    arriving = plan_shard == own_index
    arrival_order = jnp.dot(
        arriving.astype(jnp.bfloat16), before.T, preferred_element_type=jnp.float32
    ).astype(jnp.int32)
    slot_numbers = jnp.arange(capacity, dtype=jnp.int32)
    slot_match = arriving[:, None, :] & (arrival_order[:, None, :] == slot_numbers[None, :, None])
    slot_row = jnp.sum(jnp.where(slot_match, plan_row[:, None, :], 0), axis=2).reshape(-1)
    slot_live = jnp.any(slot_match, axis=2).reshape(-1)
    place_hit = slot_live[:, None] & (slot_row[:, None] == row_ids[None, :])
    lookup = jnp.sum(jnp.where(place_hit, slot_ids[:, None], 0), axis=0)
    packed = inbox_rows.reshape(slot_total, model_width)[lookup]
    normed = layer_norm(packed.astype(jnp.float32)).astype(jnp.bfloat16)
    qkv_cols, out_cols, up_cols, down_cols = (
        lax.all_gather(w_qkv, "dp", axis=1, tiled=True),
        lax.all_gather(w_out, "dp", axis=1, tiled=True),
        lax.all_gather(w_up, "dp", axis=1, tiled=True),
        lax.all_gather(w_down, "dp", axis=1, tiled=True),
    )
    weight_rows = lax.all_gather(qkv_cols, "ctx", axis=0, tiled=True)
    queries = jnp.dot(normed, weight_rows[:, :model_width], preferred_element_type=jnp.float32)
    key_pairs = jnp.dot(normed, weight_rows[:, model_width:], preferred_element_type=jnp.float32)
    queries = queries.astype(jnp.bfloat16)
    key_pairs = key_pairs.astype(jnp.bfloat16)
    key_reach = extended(key_pairs, (("ctx", 0),), seq_rows)
    seq_seg = segments[0]
    filler = jnp.full((seq_rows,), -1, jnp.int32)
    padded_seg = jnp.concatenate([filler, seq_seg, filler])
    key_seg = lax.dynamic_slice_in_dim(padded_seg, own_index * seq_rows, 3 * seq_rows, 0)
    query_seg = lax.dynamic_slice_in_dim(seq_seg, own_index * seq_rows, seq_rows, 0)
    attended = attend(queries, key_reach, query_seg, key_seg, HEADS)

    def fold_with(left_rows, weight_rows):
        return jnp.dot(left_rows, weight_rows, preferred_element_type=jnp.float32)

    projected = fold_with(attended, lax.all_gather(out_cols, "ctx", axis=0, tiled=True))
    middle = packed.astype(jnp.float32) + projected
    normed_mid = layer_norm(middle).astype(jnp.bfloat16)
    raised = fold_with(normed_mid, lax.all_gather(up_cols, "ctx", axis=0, tiled=True))
    hidden = jax.nn.gelu(raised, approximate=True).astype(jnp.bfloat16)
    lowered = fold_with(hidden, lax.all_gather(down_cols, "ctx", axis=0, tiled=True))
    result = (middle + lowered).astype(jnp.bfloat16)
    back_rows = jnp.where(slot_live[:, None], result[slot_row], jnp.zeros((), jnp.bfloat16))
    returned = lax.all_to_all(
        back_rows.reshape(shards, capacity, model_width),
        "ctx",
        split_axis=0,
        concat_axis=0,
        tiled=True,
    )
    return returned.reshape(slot_total, model_width)[outgoing_slot][None]


ANY = pl.BlockSpec(memory_space=pl.ANY)
SMEM = pl.BlockSpec(memory_space=pltpu.SMEM)
VMEM = pl.BlockSpec(memory_space=pltpu.VMEM)
VMEM_LIMIT = 56 * 2**20


def mm(left, right):
    return jnp.dot(left, right, preferred_element_type=jnp.float32)


def mm_t(left, right):
    return lax.dot_general(left, right, (((1,), (1,)), ((), ())), preferred_element_type=jnp.float32)


def spread_along(shard, chips):
    pairs = 2 * chips
    shifted = [shard]
    for step in range(1, chips):
        ring = [(i, (i + 2 * step) % pairs) for i in range(pairs)]
        shifted.append(lax.ppermute(shard, "ctx", ring))
    return shifted


def halves(shifted):
    half = len(shifted) // 2
    return jnp.stack(shifted[:half]), jnp.stack(shifted[half:])


def spread_across(own):
    near_pairs, far_pairs = ([(i, i ^ bit) for i in range(4)] for bit in (1, 2))
    near = [lax.ppermute(part, "dp", near_pairs) for part in own]
    far = [lax.ppermute(part, "dp", far_pairs) for part in own]
    cross = [lax.ppermute(near[0], "dp", far_pairs), lax.ppermute(far[1], "dp", near_pairs)]
    return list(own) + near + far + cross


def spread_cores(mine, chips):
    swap = [(i, i ^ 1) for i in range(2 * chips)]
    return mine + [lax.ppermute(part, "ctx", swap) for part in mine]


def spread(shard, chips):
    own = halves(spread_along(shard, chips))
    return spread_cores(spread_across(own), chips)


def place_tiles(buffers, where, chips, emit):
    half = chips // 2
    for index, buffer in enumerate(buffers):
        side, part = divmod(index, 8)
        bits, upper = divmod(part, 2)
        begin = half * upper
        for slot in range(begin, begin + half):
            chip = lax.rem(where[0] + (chips - slot), chips)
            core = where[1] if side == 0 else 1 - where[1]
            emit(buffer.at[slot - begin], 2 * chip + core, jnp.bitwise_xor(where[2], bits))


def place_columns(buffers, where, chips, weight, start):
    tile_rows, tile_cols = buffers[0].shape[1:]

    def put(tile, ctx, dp):
        rows = pl.ds(pl.multiple_of(ctx * tile_rows, tile_rows), tile_rows)
        cols = pl.ds(pl.multiple_of(dp * tile_cols, tile_cols), tile_cols)
        start(tile, weight.at[rows, cols])

    place_tiles(buffers, where, chips, put)


class Copies:
    def __init__(self, sem):
        self.sem = sem
        self.started = []

    def start(self, source, target):
        copy = pltpu.make_async_copy(source, target, self.sem)
        copy.start()
        self.started.append(copy)

    def wait(self):
        for copy in self.started:
            copy.wait()


def load_blocks(blocks, rows_in, start):
    offset = 0
    for block in blocks:
        start(block, rows_in.at[pl.ds(offset, block.shape[0]), :])
        offset += block.shape[0]


def project_pairs(rows_in, weight, target, base, width):
    chunk = 256

    def one(i, carry):
        rows = pl.ds(pl.multiple_of(i * chunk, chunk), chunk)
        out = pl.ds(pl.multiple_of(base + i * chunk, chunk), chunk)
        target[out, :] = mm(rows_in[rows, :], weight[:, width:]).astype(jnp.bfloat16)
        return carry

    lax.fori_loop(0, rows_in.shape[0] // chunk, one, 0)


def project_kernel(*refs, chips, heads, block_count, first):
    where, weights, blocks = refs[0], refs[1:17], refs[17 : 17 + block_count]
    outs = refs[17 + block_count :]
    if first:
        (query_out, pair_out, weight, rows_in, sem) = outs
    else:
        (pair_out, weight, rows_in, sem) = outs
    copies = Copies(sem)
    load_blocks(blocks, rows_in, copies.start)
    place_columns(weights, where, chips, weight, copies.start)
    copies.wait()
    width = rows_in.shape[1]
    if first:
        seq_rows = query_out.shape[0]
        projected = mm(rows_in[:seq_rows, :], weight[:, :width]).astype(jnp.bfloat16)
        scale = (width // heads) ** (-0.5)
        query_out[...] = (projected.astype(jnp.float32) * scale).astype(jnp.bfloat16)
    project_pairs(rows_in, weight, pair_out, 0, width)


TILE = 128
GRAIN = 16
STACK = 2


def attention_kernel(*refs, chips, heads, sizes):
    (where, bounds), weights = refs[:2], refs[2:18]
    blocks = refs[18:20]
    (near_pairs, ahead_pairs, queries, key_marks, attended) = refs[20:25]
    (weight, rows_in, pairs, picked, picked_marks, bias, sem, pair_sem) = refs[25:]
    seq_rows, width = attended.shape
    total = pairs.shape[0]
    head_dim = width // heads
    early = Copies(pair_sem)
    late = Copies(sem)
    load_blocks(blocks, rows_in, late.start)
    place_columns(weights, where, chips, weight, late.start)
    load_blocks((near_pairs, ahead_pairs), pairs, early.start)

    def clear(i, carry):
        rows = pl.ds(pl.multiple_of(i * 64, 64), 64)
        picked[rows, :] = jnp.zeros((64, 2 * width), jnp.bfloat16)
        return carry

    lax.fori_loop(0, total // 64, clear, 0)
    late.wait()
    project_pairs(rows_in, weight, pairs, total - rows_in.shape[0], width)
    early.wait()
    group = STACK * head_dim
    head_of = lax.broadcasted_iota(jnp.int32, (TILE, group), 1) // head_dim
    block_count = total // seq_rows

    def attend(size, tile_rows, used):
        def clear_marks(i, carry):
            rows = pl.ds(pl.multiple_of(i * GRAIN, GRAIN), GRAIN)
            picked_marks[rows, :] = jnp.zeros((GRAIN, 128), jnp.bfloat16)
            return carry

        lax.fori_loop(used, size // GRAIN, clear_marks, 0)
        same = mm_t(key_marks[tile_rows, :], picked_marks[:size, :])
        bias[:, :size] = jnp.where(same > 0.5, 0.0, -1e30)

        def one(i, carry):
            lanes = pl.ds(pl.multiple_of(i * group, group), group)
            value_lanes = pl.ds(pl.multiple_of(width + i * group, group), group)
            query = queries[tile_rows, lanes]
            none = jnp.zeros_like(query)
            stacked = jnp.concatenate(
                [jnp.where(head_of == j, query, none) for j in range(STACK)], 0
            )
            shift = bias[:, :size]
            scores = mm_t(stacked, picked[:size, lanes]) + jnp.concatenate([shift] * STACK, 0)
            top = jnp.max(scores, axis=-1, keepdims=True)
            expd = jnp.exp(scores - top)
            whole = jnp.sum(expd, axis=-1, keepdims=True)
            mixed = mm(expd.astype(jnp.bfloat16), picked[:size, value_lanes]) / whole
            out = jnp.where(head_of == 0, mixed[:TILE], 0.0)
            for j in range(1, STACK):
                out = jnp.where(head_of == j, mixed[j * TILE : (j + 1) * TILE], out)
            attended[tile_rows, lanes] = out.astype(jnp.bfloat16)
            return carry

        lax.fori_loop(0, width // group, one, 0)

    def one_tile(t, carry):
        tile_rows = pl.ds(pl.multiple_of(t * TILE, TILE), TILE)
        used = 0
        for index in range(block_count):
            base = index * (seq_rows // GRAIN)

            def pick(g, used, base=base):
                source = pl.ds(pl.multiple_of((base + g) * GRAIN, GRAIN), GRAIN)
                target = pl.ds(pl.multiple_of(used * GRAIN, GRAIN), GRAIN)
                picked[target, :] = pairs[source, :]
                picked_marks[target, :] = key_marks[source, :]
                return used + 1

            used = lax.fori_loop(bounds[t, 2 * index], bounds[t, 2 * index + 1], pick, used)
        floor = 0
        for size in sizes:

            @pl.when((used * GRAIN > floor) & (used * GRAIN <= size))
            def _(size=size, used=used):
                attend(size, tile_rows, used)

            floor = size
        return carry

    lax.fori_loop(0, seq_rows // TILE, one_tile, 0)


def norm_rows(values):
    row_mean = jnp.mean(values, axis=-1, keepdims=True)
    centered = values - row_mean
    variance = jnp.mean(centered * centered, axis=-1, keepdims=True)
    return centered * lax.rsqrt(variance + norm_eps)


def tail_kernel(*refs, chips, splits):
    where, weights = refs[0], refs[1:17]
    (attended, embedded, back, out_ref, w_out, w_up, w_down, middle, hidden, rows_out, sems) = refs[17:]
    tile_rows = weights[0].shape[1]
    out_cols, up_cols = splits
    folds = w_down.shape[0] // w_out.shape[0]
    stages = [Copies(sems.at[k]) for k in range(3)]

    def put(stage, column, columns, target, fold, count):
        def emit(tile, ctx, dp):
            row = pl.multiple_of((ctx * count + fold) * tile_rows, tile_rows)
            col = pl.multiple_of(dp * columns, columns)
            stages[stage].start(
                tile.at[:, pl.ds(column, columns)], target.at[pl.ds(row, tile_rows), pl.ds(col, columns)]
            )

        place_tiles(weights, where, chips, emit)

    put(0, 0, out_cols, w_out, 0, 1)
    put(1, out_cols, up_cols, w_up, 0, 1)
    for fold in range(folds):
        put(2, out_cols + up_cols + fold * out_cols, out_cols, w_down, fold, folds)
    block = 128
    count = attended.shape[0] // block

    def each(step):
        def one(i, carry):
            step(pl.ds(pl.multiple_of(i * block, block), block))
            return carry

        lax.fori_loop(0, count, one, 0)

    def project(rows):
        middle[rows, :] = embedded[rows, :].astype(jnp.float32) + mm(attended[rows, :], w_out[...])

    def raise_rows(rows):
        raised = mm(norm_rows(middle[rows, :]).astype(jnp.bfloat16), w_up[...])
        hidden[rows, :] = jax.nn.gelu(raised, approximate=True).astype(jnp.bfloat16)

    def lower(rows):
        rows_out[rows, :] = (middle[rows, :] + mm(hidden[rows, :], w_down[...])).astype(jnp.bfloat16)

    def restore(rows):
        out_ref[rows, :] = mm(back[rows, :], rows_out[...]).astype(jnp.bfloat16)

    stages[0].wait()
    each(project)
    stages[1].wait()
    each(raise_rows)
    stages[2].wait()
    each(lower)
    each(restore)


def homed_layer(
    tokens, modality, type_embed, dest_shard, dest_row, segments, w_qkv, w_out, w_up, w_down
):
    shards = lax.axis_size("ctx")
    chips = shards // 2
    ctx = lax.axis_index("ctx")
    dp = lax.axis_index("dp")
    chip, core = ctx // 2, ctx % 2
    where = jnp.stack([chip, core, dp]).astype(jnp.int32)
    seq_rows, width = tokens.shape[1:]
    qkv_width = 3 * width
    hidden_width = w_up.shape[1] * lax.axis_size("dp")
    params = pltpu.CompilerParams(vmem_limit_bytes=VMEM_LIMIT)

    qkv_parts = spread(w_qkv, chips)
    positions = (dest_shard[0] * seq_rows + dest_row[0]).astype(jnp.int32)
    numbers = jnp.arange(1, 2 * shards, dtype=jnp.int32)
    starts = jnp.sum((segments[0][None, :] < numbers[:, None]).astype(jnp.int32), axis=1)
    token_seg = jnp.sum((positions[None, :] >= starts[:, None]).astype(jnp.int32), axis=0)
    own_seg = lax.dynamic_slice_in_dim(token_seg, ctx * seq_rows, seq_rows)
    ids = jnp.arange(seq_rows, dtype=jnp.int32)
    earlier = (own_seg[None, :] < own_seg[:, None]) | (
        (own_seg[None, :] == own_seg[:, None]) & (ids[None, :] < ids[:, None])
    )
    rank = jnp.sum(earlier.astype(jnp.int32), axis=1)
    order = (rank[None, :] == ids[:, None]).astype(jnp.bfloat16)
    back = (rank[:, None] == ids[None, :]).astype(jnp.bfloat16)
    extra = jnp.where(modality[0][:, None] == 1, type_embed[1], type_embed[0]).astype(jnp.float32)
    embedded = (tokens[0].astype(jnp.float32) + extra).astype(jnp.bfloat16)
    embedded = mm(order, embedded).astype(jnp.bfloat16)
    normed = layer_norm(embedded.astype(jnp.float32)).astype(jnp.bfloat16)

    swap = [(i, i ^ 1) for i in range(shards)]
    pair_up = [(i, i ^ 2) for i in range(shards)]
    inner = [(2, 4), (3, 5), (4, 2), (5, 3)]
    outer = [(2, 0), (3, 1), (4, 6), (5, 7)]
    is_inner = (chip == 1) | (chip == 2)
    paired = lax.ppermute(normed, "ctx", pair_up)
    crossed = lax.ppermute(normed, "ctx", inner)
    crossed_pair = lax.ppermute(paired, "ctx", inner)
    passed = lax.ppermute(crossed, "ctx", outer)
    passed_pair = lax.ppermute(crossed_pair, "ctx", outer)
    ahead = jnp.where(is_inner, crossed, passed)
    behind = jnp.where(is_inner, crossed_pair, passed_pair)
    normed_other = lax.ppermute(normed, "ctx", swap)
    paired_other = lax.ppermute(paired, "ctx", swap)
    ahead_other = lax.ppermute(ahead, "ctx", swap)
    behind_other = lax.ppermute(behind, "ctx", swap)

    ahead_chip = jnp.where(chip < 2, 2, 1)
    held = [(chip, core), (chip ^ 1, core), (chip, 1 - core), (chip ^ 1, 1 - core)]
    held += [(ahead_chip, core), (ahead_chip, 1 - core), (ahead_chip ^ 1, core), (ahead_chip ^ 1, 1 - core)]
    block_seg = jnp.stack(
        [lax.dynamic_slice_in_dim(token_seg, (2 * c + k) * seq_rows, seq_rows) for c, k in held]
    )
    counts = jnp.sum((block_seg[:, None, :] < numbers[None, :, None]).astype(jnp.int32), axis=2)
    sorted_seg = jnp.sum((counts[:, :, None] <= ids[None, None, :]).astype(jnp.int32), axis=1)
    lanes = jnp.arange(128, dtype=jnp.int32)
    key_marks = (sorted_seg.reshape(-1)[:, None] == lanes[None, :]).astype(jnp.bfloat16)
    lowest = sorted_seg[0, ::TILE][:, None, None]
    highest = sorted_seg[0, TILE - 1 :: TILE][:, None, None]
    begin = jnp.sum((block_seg[None] < lowest).astype(jnp.int32), axis=2) // GRAIN
    end = (jnp.sum((block_seg[None] <= highest).astype(jnp.int32), axis=2) + GRAIN - 1) // GRAIN
    bounds = jnp.stack([begin, end], axis=2).reshape(begin.shape[0], -1)

    folds = w_down.shape[0] // w_out.shape[0]
    rest = jnp.concatenate([w_out, w_up] + jnp.split(w_down, folds), axis=1)
    row_shape = jax.ShapeDtypeStruct((seq_rows, width), jnp.bfloat16)
    total = shards * seq_rows

    def project(blocks, first=False):
        rows = len(blocks) * seq_rows
        pair_shape = jax.ShapeDtypeStruct((rows, 2 * width), jnp.bfloat16)
        return pl.pallas_call(
            functools.partial(
                project_kernel, chips=chips, heads=HEADS, block_count=len(blocks), first=first
            ),
            in_specs=[SMEM] + [ANY] * (16 + len(blocks)),
            out_shape=(row_shape, pair_shape) if first else pair_shape,
            scratch_shapes=[
                pltpu.VMEM((width, qkv_width), jnp.bfloat16),
                pltpu.VMEM((rows, width), jnp.bfloat16),
                pltpu.SemaphoreType.DMA,
            ],
            compiler_params=params,
        )(where, *qkv_parts, *blocks)

    queries, near_pairs = project((normed, paired, normed_other, paired_other), first=True)
    ahead_pairs = project((ahead, ahead_other))

    *rest_along, queries = lax.optimization_barrier((*spread_along(rest, chips), queries))
    rest_parts = spread_cores(spread_across(halves(rest_along)), chips)

    sizes = [s for s in (1024, 1280, 1536, 2048) if s < total] + [total]
    attended = pl.pallas_call(
        functools.partial(attention_kernel, chips=chips, heads=HEADS, sizes=sizes),
        in_specs=[SMEM] * 2 + [ANY] * 20 + [VMEM] * 2,
        out_shape=row_shape,
        scratch_shapes=[
            pltpu.VMEM((width, qkv_width), jnp.bfloat16),
            pltpu.VMEM((2 * seq_rows, width), jnp.bfloat16),
            pltpu.VMEM((total, 2 * width), jnp.bfloat16),
            pltpu.VMEM((total, 2 * width), jnp.bfloat16),
            pltpu.VMEM((total, 128), jnp.bfloat16),
            pltpu.VMEM((TILE, total), jnp.float32),
            pltpu.SemaphoreType.DMA,
            pltpu.SemaphoreType.DMA,
        ],
        compiler_params=params,
        name="attend",
    )(where, bounds, *qkv_parts, behind, behind_other, near_pairs, ahead_pairs, queries, key_marks)
    result = pl.pallas_call(
        functools.partial(tail_kernel, chips=chips, splits=(w_out.shape[1], w_up.shape[1])),
        in_specs=[SMEM] + [ANY] * 16 + [VMEM] * 3,
        out_shape=row_shape,
        scratch_shapes=[
            pltpu.VMEM((width, width), jnp.bfloat16),
            pltpu.VMEM((width, hidden_width), jnp.bfloat16),
            pltpu.VMEM((hidden_width, width), jnp.bfloat16),
            pltpu.VMEM((seq_rows, width), jnp.float32),
            pltpu.VMEM((seq_rows, hidden_width), jnp.bfloat16),
            pltpu.VMEM((seq_rows, width), jnp.bfloat16),
            pltpu.SemaphoreType.DMA((3,)),
        ],
        compiler_params=params,
        name="tail",
    )(where, *rest_parts, attended, embedded, back)
    return result[None]


def solution(mesh):
    placed = (
        P("dp", "ctx", None),
        P("dp", "ctx"),
        P(),
        P("dp", None),
        P("dp", None),
        P("dp", None),
        P("ctx", "dp"),
        P("ctx", "dp"),
        P("ctx", "dp"),
        P("ctx", "dp"),
    )
    small = mesh.shape["ctx"] == 8 and mesh.shape["dp"] == 4

    def layer(*args):
        return (homed_layer if small else packed_layer)(*args)

    return jax.shard_map(
        layer, mesh=mesh, in_specs=placed, out_specs=P("dp", "ctx", None), check_vma=False
    )
```

```python
import functools

import jax
import jax.numpy as jnp
from jax import lax
from jax.experimental import pallas as pl
from jax.experimental.pallas import tpu as pltpu
from jax.sharding import PartitionSpec as P


HEADS = 16


norm_eps = 1e-06


def extended(value, sides, width):
    for axis, dim in sides:
        devices, length = (lax.axis_size(axis), value.shape[dim])
        up = [(i, (i + 1) % devices) for i in range(devices - 1)]
        down = [(j, i) for i, j in up]
        last = lax.slice_in_dim(value, length - width, length, axis=dim)
        initial = lax.slice_in_dim(value, 0, width, axis=dim)
        before = lax.ppermute(last, axis, up)
        after = lax.ppermute(initial, axis, down)
        value = jnp.concatenate([before, value, after], axis=dim)
    return value


def layer_norm(values):
    row_mean = jnp.mean(values, axis=-1, keepdims=True)
    centered = values - row_mean
    spread = jnp.mean(centered * centered, axis=-1, keepdims=True)
    return centered * lax.rsqrt(spread + norm_eps)


def attend(queries, key_pairs, query_seg, key_seg, head_count):
    seq_rows, model_width = queries.shape
    key_span = key_pairs.shape[0]
    groups = head_count // 4
    head_dim = model_width // head_count
    query_groups = queries.reshape(seq_rows, groups, 4, head_dim).transpose(1, 0, 2, 3)
    key_groups = (
        key_pairs[:, :model_width].reshape(key_span, groups, 4, head_dim).transpose(1, 0, 2, 3)
    )
    value_groups = (
        key_pairs[:, model_width:].reshape(key_span, groups, 4, head_dim).transpose(1, 0, 2, 3)
    )
    allowed = query_seg[:, None] == key_seg[None, :]
    score_scale = head_dim ** (-0.5)

    def one_group(operands):
        query_part, key_part, value_part = operands
        scores = (
            jnp.einsum("qhd,khd->hqk", query_part, key_part, preferred_element_type=jnp.float32)
            * score_scale
        )
        scores = jnp.where(allowed[None], scores, -1e30)
        row_max = jnp.max(scores, axis=-1, keepdims=True)
        expd = jnp.exp(scores - row_max)
        attn_probs = (expd / jnp.sum(expd, axis=-1, keepdims=True)).astype(jnp.bfloat16)
        return jnp.einsum(
            "hqk,khd->qhd", attn_probs, value_part, preferred_element_type=jnp.float32
        )

    head_mix = lax.map(one_group, (query_groups, key_groups, value_groups))
    return head_mix.transpose(1, 0, 2, 3).reshape(seq_rows, model_width).astype(jnp.bfloat16)


def packed_layer(tokens, modality, type_embed, dest_shard, dest_row, segments, w_qkv, w_out, w_up, w_down):
    shards = lax.axis_size("ctx")
    own_index = lax.axis_index("ctx")
    seq_rows = tokens.shape[1]
    model_width = tokens.shape[2]
    capacity = 2 * seq_rows // shards
    slot_total = shards * capacity
    extra = jnp.where(modality[0][:, None] == 1, type_embed[1], type_embed[0]).astype(jnp.float32)
    embedded = (tokens[0].astype(jnp.float32) + extra).astype(jnp.bfloat16)
    plan_shard = dest_shard[0].reshape(shards, seq_rows)
    plan_row = dest_row[0].reshape(shards, seq_rows)
    owners = jnp.arange(shards, dtype=jnp.int32)
    row_ids = jnp.arange(seq_rows, dtype=jnp.int32)
    slot_ids = jnp.arange(slot_total, dtype=jnp.int32)
    before = (row_ids[:, None] > row_ids[None, :]).astype(jnp.bfloat16)
    own_plan = lax.dynamic_index_in_dim(plan_shard, own_index, 0, keepdims=False)
    chosen = own_plan[:, None] == owners[None, :]
    earlier_all = jnp.dot(before, chosen.astype(jnp.bfloat16), preferred_element_type=jnp.float32)
    earlier = jnp.sum(jnp.where(chosen, earlier_all, 0.0), axis=1).astype(jnp.int32)
    outgoing_slot = own_plan * capacity + earlier
    slot_hit = outgoing_slot[None, :] == slot_ids[:, None]
    slot_token = jnp.sum(jnp.where(slot_hit, row_ids[None, :], 0), axis=1)
    slot_full = jnp.any(slot_hit, axis=1)
    outbox_rows = jnp.where(slot_full[:, None], embedded[slot_token], jnp.zeros((), jnp.bfloat16))
    inbox_rows = lax.all_to_all(
        outbox_rows.reshape(shards, capacity, model_width),
        "ctx",
        split_axis=0,
        concat_axis=0,
        tiled=True,
    )
    arriving = plan_shard == own_index
    arrival_order = jnp.dot(
        arriving.astype(jnp.bfloat16), before.T, preferred_element_type=jnp.float32
    ).astype(jnp.int32)
    slot_numbers = jnp.arange(capacity, dtype=jnp.int32)
    slot_match = arriving[:, None, :] & (arrival_order[:, None, :] == slot_numbers[None, :, None])
    slot_row = jnp.sum(jnp.where(slot_match, plan_row[:, None, :], 0), axis=2).reshape(-1)
    slot_live = jnp.any(slot_match, axis=2).reshape(-1)
    place_hit = slot_live[:, None] & (slot_row[:, None] == row_ids[None, :])
    lookup = jnp.sum(jnp.where(place_hit, slot_ids[:, None], 0), axis=0)
    packed = inbox_rows.reshape(slot_total, model_width)[lookup]
    normed = layer_norm(packed.astype(jnp.float32)).astype(jnp.bfloat16)
    qkv_cols, out_cols, up_cols, down_cols = (
        lax.all_gather(w_qkv, "dp", axis=1, tiled=True),
        lax.all_gather(w_out, "dp", axis=1, tiled=True),
        lax.all_gather(w_up, "dp", axis=1, tiled=True),
        lax.all_gather(w_down, "dp", axis=1, tiled=True),
    )
    weight_rows = lax.all_gather(qkv_cols, "ctx", axis=0, tiled=True)
    queries = jnp.dot(normed, weight_rows[:, :model_width], preferred_element_type=jnp.float32)
    key_pairs = jnp.dot(normed, weight_rows[:, model_width:], preferred_element_type=jnp.float32)
    queries = queries.astype(jnp.bfloat16)
    key_pairs = key_pairs.astype(jnp.bfloat16)
    key_reach = extended(key_pairs, (("ctx", 0),), seq_rows)
    seq_seg = segments[0]
    filler = jnp.full((seq_rows,), -1, jnp.int32)
    padded_seg = jnp.concatenate([filler, seq_seg, filler])
    key_seg = lax.dynamic_slice_in_dim(padded_seg, own_index * seq_rows, 3 * seq_rows, 0)
    query_seg = lax.dynamic_slice_in_dim(seq_seg, own_index * seq_rows, seq_rows, 0)
    attended = attend(queries, key_reach, query_seg, key_seg, HEADS)

    def fold_with(left_rows, weight_rows):
        return jnp.dot(left_rows, weight_rows, preferred_element_type=jnp.float32)

    projected = fold_with(attended, lax.all_gather(out_cols, "ctx", axis=0, tiled=True))
    middle = packed.astype(jnp.float32) + projected
    normed_mid = layer_norm(middle).astype(jnp.bfloat16)
    raised = fold_with(normed_mid, lax.all_gather(up_cols, "ctx", axis=0, tiled=True))
    hidden = jax.nn.gelu(raised, approximate=True).astype(jnp.bfloat16)
    lowered = fold_with(hidden, lax.all_gather(down_cols, "ctx", axis=0, tiled=True))
    result = (middle + lowered).astype(jnp.bfloat16)
    back_rows = jnp.where(slot_live[:, None], result[slot_row], jnp.zeros((), jnp.bfloat16))
    returned = lax.all_to_all(
        back_rows.reshape(shards, capacity, model_width),
        "ctx",
        split_axis=0,
        concat_axis=0,
        tiled=True,
    )
    return returned.reshape(slot_total, model_width)[outgoing_slot][None]


ANY = pl.BlockSpec(memory_space=pl.ANY)
SMEM = pl.BlockSpec(memory_space=pltpu.SMEM)
VMEM = pl.BlockSpec(memory_space=pltpu.VMEM)


def vmem(mebibytes):
    return pltpu.CompilerParams(vmem_limit_bytes=mebibytes * 2**20)


def mm(left, right):
    return jnp.dot(left, right, preferred_element_type=jnp.float32)


def mm_t(left, right):
    return lax.dot_general(left, right, (((1,), (1,)), ((), ())), preferred_element_type=jnp.float32)


def spread_along(shard, chips):
    pairs = 2 * chips
    shifted = [shard]
    for step in range(1, chips):
        ring = [(i, (i + 2 * step) % pairs) for i in range(pairs)]
        shifted.append(lax.ppermute(shard, "ctx", ring))
    return shifted


def halves(shifted):
    half = len(shifted) // 2
    return jnp.stack(shifted[:half]), jnp.stack(shifted[half:])


def spread_across(own, meanwhile=()):
    near_pairs, far_pairs = ([(i, i ^ bit) for i in range(4)] for bit in (1, 2))
    near = [lax.ppermute(part, "dp", near_pairs) for part in own]
    far = [lax.ppermute(part, "dp", far_pairs) for part in own]
    (near[0], *meanwhile) = lax.optimization_barrier((near[0], *meanwhile))
    cross = [lax.ppermute(near[0], "dp", far_pairs), lax.ppermute(far[1], "dp", near_pairs)]
    return list(own) + near + far + cross, meanwhile


def spread_cores(mine, chips):
    swap = [(i, i ^ 1) for i in range(2 * chips)]
    return mine + [lax.ppermute(part, "ctx", swap) for part in mine]


def place_tiles(buffers, where, chips, emit):
    half = chips // 2
    for index, buffer in enumerate(buffers):
        side, part = divmod(index, 8)
        bits, upper = divmod(part, 2)
        begin = half * upper
        for slot in range(begin, begin + half):
            chip = lax.rem(where[0] + (chips - slot), chips)
            core = where[1] if side == 0 else 1 - where[1]
            emit(buffer.at[slot - begin], 2 * chip + core, jnp.bitwise_xor(where[2], bits))


def place_columns(buffers, where, chips, weight, start):
    tile_rows, tile_cols = buffers[0].shape[1:]

    def put(tile, ctx, dp):
        rows = pl.ds(pl.multiple_of(ctx * tile_rows, tile_rows), tile_rows)
        cols = pl.ds(pl.multiple_of(dp * tile_cols, tile_cols), tile_cols)
        start(tile, weight.at[rows, cols])

    place_tiles(buffers, where, chips, put)


class Copies:
    def __init__(self, sem):
        self.sem = sem
        self.started = []

    def start(self, source, target):
        copy = pltpu.make_async_copy(source, target, self.sem)
        copy.start()
        self.started.append(copy)

    def wait(self):
        for copy in self.started:
            copy.wait()


def load_blocks(blocks, rows_in, start):
    offset = 0
    for block in blocks:
        start(block, rows_in.at[pl.ds(offset, block.shape[0]), :])
        offset += block.shape[0]


def project_pairs(rows_in, weight, target, width, base_of=None):
    chunk = 192 if base_of else 256

    def one(i, carry):
        rows = pl.ds(pl.multiple_of(i * chunk, chunk), chunk)
        out = pl.ds(pl.multiple_of(base_of(i * chunk), chunk), chunk) if base_of else rows
        target[out, :] = mm(rows_in[rows, :], weight[:, width:]).astype(jnp.bfloat16)
        return carry

    lax.fori_loop(0, rows_in.shape[0] // chunk, one, 0)


def project_kernel(*refs, chips, heads, block_count, first):
    where, weights, blocks = refs[0], refs[1:17], refs[17 : 17 + block_count]
    outs = refs[17 + block_count :]
    if first:
        (query_out, pair_out, weight, rows_in, sem) = outs
    else:
        (pair_out, weight, rows_in, sem) = outs
    copies = Copies(sem)
    load_blocks(blocks, rows_in, copies.start)
    place_columns(weights, where, chips, weight, copies.start)
    copies.wait()
    width = rows_in.shape[1]
    if first:
        seq_rows = query_out.shape[0]
        projected = mm(rows_in[:seq_rows, :], weight[:, :width]).astype(jnp.bfloat16)
        scale = (width // heads) ** (-0.5)
        query_out[...] = (projected.astype(jnp.float32) * scale).astype(jnp.bfloat16)
    project_pairs(rows_in, weight, pair_out, width)


TILE = 128
GRAIN = 16
STACK = 2
EXCLUDED = -1e30


def attention_kernel(*refs, chips, heads, sizes):
    (where, bounds), weights = refs[:2], refs[2:18]
    blocks = refs[18:20]
    (near_pairs, ahead_pairs, queries, key_marks, attended) = refs[20:25]
    (weight, rows_in, pairs, picked, picked_marks, sem, pair_sem) = refs[25:]
    seq_rows, width = attended.shape
    total = pairs.shape[0]
    head_dim = width // heads
    chip, core, ahead = where[0], where[1], where[3]
    beside, behind = jnp.bitwise_xor(chip, 1), jnp.bitwise_xor(ahead, 1)

    def row_of(chip_index, core_index):
        return pl.multiple_of((2 * chip_index + core_index) * seq_rows, seq_rows)

    early = Copies(pair_sem)
    late = Copies(sem)
    load_blocks(blocks, rows_in, late.start)
    place_columns(weights, where, chips, weight, late.start)

    def keep(source, index, chip_index, core_index):
        early.start(
            source.at[pl.ds(index * seq_rows, seq_rows), :],
            pairs.at[pl.ds(row_of(chip_index, core_index), seq_rows), :],
        )

    for index, (c, k) in enumerate(((chip, core), (beside, core), (chip, 1 - core), (beside, 1 - core))):
        keep(near_pairs, index, c, k)
    for index, k in enumerate((core, 1 - core)):
        keep(ahead_pairs, index, ahead, k)

    def clear(i, carry):
        rows = pl.ds(pl.multiple_of(i * 64, 64), 64)
        picked[rows, :] = jnp.zeros((64, 2 * width), jnp.bfloat16)
        return carry

    lax.fori_loop(0, total // 64, clear, 0)
    late.wait()

    def base_of(row):
        mine = row < seq_rows
        return row_of(behind, jnp.where(mine, core, 1 - core)) + jnp.where(mine, row, row - seq_rows)

    project_pairs(rows_in, weight, pairs, width, base_of)
    early.wait()
    group = STACK * head_dim
    head_of = lax.broadcasted_iota(jnp.int32, (TILE, group), 1) // head_dim
    block_count = total // seq_rows
    own_row = row_of(chip, core)

    def attend(size, t, used):
        tile_rows = pl.ds(pl.multiple_of(t * TILE, TILE), TILE)

        def exclude(i, carry):
            rows = pl.ds(pl.multiple_of(i * GRAIN, GRAIN), GRAIN)
            picked_marks[rows, :] = jnp.full((GRAIN, 128), EXCLUDED, jnp.bfloat16)
            return carry

        lax.fori_loop(used, size // GRAIN, exclude, 0)
        own_marks = key_marks[pl.ds(pl.multiple_of(own_row + t * TILE, TILE), TILE), :]
        own_marks = jnp.where(own_marks.astype(jnp.float32) == 0, 1.0, 0.0).astype(jnp.bfloat16)
        own_marks = jnp.concatenate([own_marks] * STACK, 0)

        def one(i, carry):
            lanes = pl.ds(pl.multiple_of(i * group, group), group)
            value_lanes = pl.ds(pl.multiple_of(width + i * group, group), group)
            query = queries[tile_rows, lanes]
            none = jnp.zeros_like(query)
            stacked = jnp.concatenate(
                [jnp.where(head_of == j, query, none) for j in range(STACK)], 0
            )
            scores = mm_t(
                jnp.concatenate([stacked, own_marks], 1),
                jnp.concatenate([picked[:size, lanes], picked_marks[:size, :]], 1),
            )
            top = jnp.max(scores, axis=-1, keepdims=True)
            expd = jnp.exp(scores - top)
            whole = jnp.sum(expd, axis=-1, keepdims=True)
            mixed = mm(expd.astype(jnp.bfloat16), picked[:size, value_lanes]) / whole
            out = mixed[:TILE]
            for j in range(1, STACK):
                out = jnp.where(head_of == j, mixed[j * TILE : (j + 1) * TILE], out)
            attended[tile_rows, lanes] = out.astype(jnp.bfloat16)
            return carry

        lax.fori_loop(0, width // group, one, 0, unroll=UNROLL)

    def one_tile(t, carry):
        used = 0
        for index in range(block_count):
            base = index * (seq_rows // GRAIN)

            def pick(g, used, base=base):
                source = pl.ds(pl.multiple_of((base + g) * GRAIN, GRAIN), GRAIN)
                target = pl.ds(pl.multiple_of(used * GRAIN, GRAIN), GRAIN)
                picked[target, :] = pairs[source, :]
                picked_marks[target, :] = key_marks[source, :]
                return used + 1

            used = lax.fori_loop(bounds[t, 2 * index], bounds[t, 2 * index + 1], pick, used)
        floor = 0
        for size in sizes:

            @pl.when((used * GRAIN > floor) & (used * GRAIN <= size))
            def _(size=size, used=used):
                attend(size, t, used)

            floor = size
        return carry

    lax.fori_loop(0, seq_rows // TILE, one_tile, 0)


UNROLL = 2


def norm_rows(values):
    row_mean = jnp.mean(values, axis=-1, keepdims=True)
    centered = values - row_mean
    variance = jnp.mean(centered * centered, axis=-1, keepdims=True)
    return centered * lax.rsqrt(variance + norm_eps)


def tail_kernel(*refs, chips, splits):
    where, weights = refs[0], refs[1:17]
    (attended, embedded, back, out_ref, w_out, w_up, w_down, middle, hidden, rows_out, sems) = refs[17:]
    tile_rows = weights[0].shape[1]
    out_cols, up_cols = splits
    folds = w_down.shape[0] // w_out.shape[0]
    stages = [Copies(sems.at[k]) for k in range(3)]

    def put(stage, column, columns, target, fold, count):
        def emit(tile, ctx, dp):
            row = pl.multiple_of((ctx * count + fold) * tile_rows, tile_rows)
            col = pl.multiple_of(dp * columns, columns)
            stages[stage].start(
                tile.at[:, pl.ds(column, columns)], target.at[pl.ds(row, tile_rows), pl.ds(col, columns)]
            )

        place_tiles(weights, where, chips, emit)

    put(0, 0, out_cols, w_out, 0, 1)
    put(1, out_cols, up_cols, w_up, 0, 1)
    for fold in range(folds):
        put(2, out_cols + up_cols + fold * out_cols, out_cols, w_down, fold, folds)
    block = 128
    count = attended.shape[0] // block

    def each(step):
        def one(i, carry):
            step(pl.ds(pl.multiple_of(i * block, block), block))
            return carry

        lax.fori_loop(0, count, one, 0)

    def project(rows):
        middle[rows, :] = embedded[rows, :].astype(jnp.float32) + mm(attended[rows, :], w_out[...])

    def raise_rows(rows):
        raised = mm(norm_rows(middle[rows, :]).astype(jnp.bfloat16), w_up[...])
        hidden[rows, :] = jax.nn.gelu(raised, approximate=True).astype(jnp.bfloat16)

    def lower(rows):
        rows_out[rows, :] = (middle[rows, :] + mm(hidden[rows, :], w_down[...])).astype(jnp.bfloat16)

    def restore(rows):
        out_ref[rows, :] = mm(back[rows, :], rows_out[...]).astype(jnp.bfloat16)

    stages[0].wait()
    each(project)
    stages[1].wait()
    each(raise_rows)
    stages[2].wait()
    each(lower)
    each(restore)


def homed_layer(
    tokens, modality, type_embed, dest_shard, dest_row, segments, w_qkv, w_out, w_up, w_down
):
    shards = lax.axis_size("ctx")
    chips = shards // 2
    ctx = lax.axis_index("ctx")
    dp = lax.axis_index("dp")
    chip, core = ctx // 2, ctx % 2
    where = jnp.stack([chip, core, dp, jnp.where(chip < 2, 2, 1)]).astype(jnp.int32)
    seq_rows, width = tokens.shape[1:]
    qkv_width = 3 * width
    hidden_width = w_up.shape[1] * lax.axis_size("dp")

    positions = (dest_shard[0] * seq_rows + dest_row[0]).astype(jnp.int32)
    numbers = jnp.arange(1, 2 * shards, dtype=jnp.int32)
    starts = jnp.sum((segments[0][None, :] < numbers[:, None]).astype(jnp.int32), axis=1)
    token_seg = jnp.sum((positions[None, :] >= starts[:, None]).astype(jnp.int32), axis=0)
    block_seg = token_seg.reshape(shards, seq_rows)
    own_seg = lax.dynamic_index_in_dim(block_seg, ctx, 0, keepdims=False)
    ids = jnp.arange(seq_rows, dtype=jnp.int32)
    earlier = (own_seg[None, :] < own_seg[:, None]) | (
        (own_seg[None, :] == own_seg[:, None]) & (ids[None, :] < ids[:, None])
    )
    rank = jnp.sum(earlier.astype(jnp.int32), axis=1)
    order = (rank[None, :] == ids[:, None]).astype(jnp.bfloat16)
    back = (rank[:, None] == ids[None, :]).astype(jnp.bfloat16)
    extra = jnp.where(modality[0][:, None] == 1, type_embed[1], type_embed[0]).astype(jnp.float32)
    embedded = (tokens[0].astype(jnp.float32) + extra).astype(jnp.bfloat16)
    embedded = mm(order, embedded).astype(jnp.bfloat16)
    normed = layer_norm(embedded.astype(jnp.float32)).astype(jnp.bfloat16)

    counts = jnp.sum((block_seg[:, None, :] < numbers[None, :, None]).astype(jnp.int32), axis=2)
    sorted_seg = jnp.sum((counts[:, :, None] <= ids[None, None, :]).astype(jnp.int32), axis=1)
    lanes = jnp.arange(128, dtype=jnp.int32)
    key_marks = jnp.where(sorted_seg.reshape(-1)[:, None] == lanes[None, :], 0.0, EXCLUDED)
    key_marks = key_marks.astype(jnp.bfloat16)
    own_counts = jnp.sum((own_seg[None, :] < numbers[:, None]).astype(jnp.int32), axis=1)
    first_rows = TILE * jnp.arange(seq_rows // TILE, dtype=jnp.int32)

    def seg_at(rows):
        return jnp.sum((own_counts[None, :] <= rows[:, None]).astype(jnp.int32), axis=1)[:, None, None]

    begin = jnp.sum((block_seg[None] < seg_at(first_rows)).astype(jnp.int32), axis=2) // GRAIN
    end = jnp.sum((block_seg[None] <= seg_at(first_rows + TILE - 1)).astype(jnp.int32), axis=2)
    end = (end + GRAIN - 1) // GRAIN
    bounds = jnp.stack([begin, end], axis=2).reshape(begin.shape[0], -1)

    qkv_own = halves(spread_along(w_qkv, chips))
    qkv_parts, (key_marks, bounds) = spread_across(qkv_own, (key_marks, bounds))
    qkv_parts = spread_cores(qkv_parts, chips)

    swap = [(i, i ^ 1) for i in range(shards)]
    pair_up = [(i, i ^ 2) for i in range(shards)]
    inner = [(2, 4), (3, 5), (4, 2), (5, 3)]
    outer = [(2, 0), (3, 1), (4, 6), (5, 7)]
    is_inner = (chip == 1) | (chip == 2)
    paired = lax.ppermute(normed, "ctx", pair_up)
    crossed = lax.ppermute(normed, "ctx", inner)
    crossed_pair = lax.ppermute(paired, "ctx", inner)
    passed = lax.ppermute(crossed, "ctx", outer)
    passed_pair = lax.ppermute(crossed_pair, "ctx", outer)
    ahead = jnp.where(is_inner, crossed, passed)
    behind = jnp.where(is_inner, crossed_pair, passed_pair)
    normed_other = lax.ppermute(normed, "ctx", swap)
    paired_other = lax.ppermute(paired, "ctx", swap)
    ahead_other = lax.ppermute(ahead, "ctx", swap)
    behind_other = lax.ppermute(behind, "ctx", swap)

    folds = w_down.shape[0] // w_out.shape[0]
    rest = jnp.concatenate([w_out, w_up] + jnp.split(w_down, folds), axis=1)
    row_shape = jax.ShapeDtypeStruct((seq_rows, width), jnp.bfloat16)
    total = shards * seq_rows

    def project(blocks, first=False):
        rows = len(blocks) * seq_rows
        pair_shape = jax.ShapeDtypeStruct((rows, 2 * width), jnp.bfloat16)
        return pl.pallas_call(
            functools.partial(
                project_kernel, chips=chips, heads=HEADS, block_count=len(blocks), first=first
            ),
            in_specs=[SMEM] + [ANY] * (16 + len(blocks)),
            out_shape=(row_shape, pair_shape) if first else pair_shape,
            scratch_shapes=[
                pltpu.VMEM((width, qkv_width), jnp.bfloat16),
                pltpu.VMEM((rows, width), jnp.bfloat16),
                pltpu.SemaphoreType.DMA,
            ],
            compiler_params=vmem(26),
        )(where, *qkv_parts, *blocks)

    queries, near_pairs = project((normed, paired, normed_other, paired_other), first=True)
    ahead_pairs = project((ahead, ahead_other))

    *rest_along, queries = lax.optimization_barrier((*spread_along(rest, chips), queries))
    rest_parts = spread_cores(spread_across(halves(rest_along))[0], chips)

    sizes = [s for s in (1024, 1280, 1408, 1536, 2048) if s < total] + [total]
    attended = pl.pallas_call(
        functools.partial(attention_kernel, chips=chips, heads=HEADS, sizes=sizes),
        in_specs=[SMEM] * 2 + [ANY] * 20 + [VMEM] * 2,
        out_shape=row_shape,
        scratch_shapes=[
            pltpu.VMEM((width, qkv_width), jnp.bfloat16),
            pltpu.VMEM((2 * seq_rows, width), jnp.bfloat16),
            pltpu.VMEM((total, 2 * width), jnp.bfloat16),
            pltpu.VMEM((total, 2 * width), jnp.bfloat16),
            pltpu.VMEM((total, 128), jnp.bfloat16),
            pltpu.SemaphoreType.DMA,
            pltpu.SemaphoreType.DMA,
        ],
        compiler_params=vmem(46),
        name="attend",
    )(where, bounds, *qkv_parts, behind, behind_other, near_pairs, ahead_pairs, queries, key_marks)
    result = pl.pallas_call(
        functools.partial(tail_kernel, chips=chips, splits=(w_out.shape[1], w_up.shape[1])),
        in_specs=[SMEM] + [ANY] * 16 + [VMEM] * 3,
        out_shape=row_shape,
        scratch_shapes=[
            pltpu.VMEM((width, width), jnp.bfloat16),
            pltpu.VMEM((width, hidden_width), jnp.bfloat16),
            pltpu.VMEM((hidden_width, width), jnp.bfloat16),
            pltpu.VMEM((seq_rows, width), jnp.float32),
            pltpu.VMEM((seq_rows, hidden_width), jnp.bfloat16),
            pltpu.VMEM((seq_rows, width), jnp.bfloat16),
            pltpu.SemaphoreType.DMA((3,)),
        ],
        compiler_params=vmem(26),
        name="tail",
    )(where, *rest_parts, attended, embedded, back)
    return result[None]


def solution(mesh):
    placed = (
        P("dp", "ctx", None),
        P("dp", "ctx"),
        P(),
        P("dp", None),
        P("dp", None),
        P("dp", None),
        P("ctx", "dp"),
        P("ctx", "dp"),
        P("ctx", "dp"),
        P("ctx", "dp"),
    )
    small = mesh.shape["ctx"] == 8 and mesh.shape["dp"] == 4

    def layer(*args):
        return (homed_layer if small else packed_layer)(*args)

    return jax.shard_map(
        layer, mesh=mesh, in_specs=placed, out_specs=P("dp", "ctx", None), check_vma=False
    )
```
